128 devices in a mesh: row: 8 (over z, y_hi), col: 16 (over x, y_lo, core).
Axes of the slice: x: 4, y: 4 (y_hi: 2, y_lo: 2; y = y_hi * 2 + y_lo), z: 4, core: 2. Of those that a mesh axis runs over, the one named last changes fastest.
Arguments:
- tri_panels: float32 [8192, 8192], P('row', 'col'), may hold values from -1 to 2, as said below
- rhs_rows: float32 [8192, 2048], P(('row', 'col')), may hold values from -6 to 6
Outputs:
- rhs_grid: float32 [8192, 2048], P('row', 'col')
The draws below stay inside these ranges and needn't reach their ends.
Inputs may be any that keep to these rules, and one draw needn't show every extreme that they name: `tri_panels`: in L's row order the entries above the diagonal are zero and the diagonal entries are positive.
All inputs are finite; a program needn't handle non-finite values.
Results may differ from the reference program's by a relative error of at most 0.00011.
Values sent between devices are 32-bit elements; how exact they have to be, the bound alone decides.
A program may use at most 256 MiB of HBM per device.

```python
import math
import jax
import jax.numpy as jnp
from jax import lax

N = 8192
NB = 512
NRHS = 2048
K = 8192
N_ROW = 8
N_COL = 16


def draw_tri_panels(key, part):
    key_offdiag = jax.random.fold_in(key, 11)
    key_diagonal = jax.random.fold_in(key, 23)
    bound_value = 2.7 / math.sqrt(N)
    off_diagonal = jax.random.uniform(key_offdiag, (N, K), jnp.float32, -bound_value, bound_value)
    diagonal_values = jnp.exp(jax.random.uniform(key_diagonal, (N,), jnp.float32, 0.0, math.log(2.0)))
    row_index = jnp.arange(N, dtype=jnp.int32)[:, None]
    col_index = jnp.arange(K, dtype=jnp.int32)[None, :]
    matrix_lower = jnp.where(row_index > col_index, off_diagonal, jnp.float32(0.0))
    matrix_lower = jnp.where(row_index == col_index, diagonal_values[:, None], matrix_lower)
    block_count = N // (N_ROW * NB)
    return matrix_lower.reshape(block_count, N_ROW, NB, K).transpose(1, 0, 2, 3).reshape(N, K)


def level_of(rng, shape, cuts, least, high):
    def one(axis_at, parts):
        steps = jax.random.uniform(jax.random.fold_in(jax.random.fold_in(rng, 6), axis_at), (parts,), jnp.float32, least / len(cuts), high / len(cuts))
        return jnp.repeat(jnp.exp(steps), shape[axis_at] // parts).reshape((-1,) + (1,) * (len(shape) - axis_at - 1))

    gain = one(*cuts[0])
    for cut in cuts[1:]:
        gain = gain * one(*cut)
    return gain


def normal_values(key, extent, deviation, most, pieces=(), kind=jnp.bfloat16):
    factor_of = level_of(key, extent, pieces, -0.22, 0.18) if pieces else 1.0
    drawn = jax.random.normal(key, extent, jnp.float32) * deviation * factor_of
    return jnp.minimum(jnp.maximum(drawn, -most), most).astype(kind)


def setup_inputs(seed: int = 0) -> dict:
    splits = jax.random.split(jax.random.key(seed), 3)
    return {
        "tri_panels": draw_tri_panels(jax.random.fold_in(splits[2], 71), 0),
        "rhs_rows": normal_values(splits[1], (N, NRHS), 1.0, 6.0, ((0, 128),), jnp.float32),
    }


def reference(tri_panels, rhs_rows):
    block_count = N // (N_ROW * NB)
    sub_rows = NB // N_COL
    lower_full = tri_panels.reshape(N_ROW, block_count, NB, K).transpose(1, 0, 2, 3).reshape(N, K)
    right_side = rhs_rows.reshape(N_ROW, N_COL, block_count, sub_rows, NRHS).transpose(2, 0, 1, 3, 4).reshape(N, NRHS)
    for step_index in range(N_COL):
        top_row = step_index * NB
        bottom = top_row + NB
        solution = jax.scipy.linalg.solve_triangular(lower_full[top_row:bottom, top_row:bottom], right_side[top_row:bottom], lower=True)
        below_rows = right_side[bottom:] - jnp.dot(lower_full[bottom:, top_row:bottom].astype(jnp.float32), solution.astype(jnp.float32), precision=lax.Precision.HIGHEST, preferred_element_type=jnp.float32)
        right_side = jnp.concatenate([right_side[:top_row], solution, below_rows], 0)
    return right_side.reshape(block_count, N_ROW, NB, NRHS).transpose(1, 0, 2, 3).reshape(N, NRHS)
```

```python
import functools

import jax
import jax.numpy as jnp
from jax import lax
from jax.experimental import pallas as pl
from jax.experimental.pallas import tpu as pltpu
from jax.sharding import PartitionSpec as P

MESH = pl.DeviceIdType.MESH
F32 = jnp.float32
PIECES = 2
HIGH = lax.Precision.HIGHEST


def split(a):
    top = a.astype(jnp.bfloat16)
    return top, (a - top.astype(F32)).astype(jnp.bfloat16)


def product(a, b):
    a_top, a_rest = split(a)
    b_top, b_rest = split(b)
    dot = functools.partial(jnp.dot, preferred_element_type=F32)
    return dot(a_top, b_top) + (dot(a_top, b_rest) + dot(a_rest, b_top))


def exact(a, b):
    return jnp.dot(a, b, precision=HIGH, preferred_element_type=F32)


def invert(a_ref, w_ref):
    size = a_ref.shape[0]
    base = min(32, size)
    group = min(128, size)
    w_ref[...] = jnp.zeros_like(w_ref)
    eye = (
        lax.broadcasted_iota(jnp.int32, (base, base), 0)
        == lax.broadcasted_iota(jnp.int32, (base, base), 1)
    )
    for first in range(0, size, group):
        spots = list(range(first, first + group, base))
        scaled, scales, solved = [], [], []
        for spot in spots:
            a = a_ref[spot : spot + base, spot : spot + base]
            diag = jnp.where(eye, a, 0.0)
            inv_col = 1.0 / jnp.sum(diag, axis=1, keepdims=True)
            scales.append(1.0 / jnp.sum(diag, axis=0, keepdims=True))
            scaled.append(jnp.where(eye, 0.0, a * inv_col))
            solved.append(jnp.where(eye, jnp.ones((), F32), jnp.zeros((), F32)))
        for i in range(base - 1):
            for n in range(len(spots)):
                solved[n] = solved[n] - scaled[n][:, i : i + 1] * solved[n][i : i + 1, :]
        for n, spot in enumerate(spots):
            w_ref[spot : spot + base, spot : spot + base] = solved[n] * scales[n]
    half = base
    while half < group:
        i = lax.broadcasted_iota(jnp.int32, (group, group), 0) // half
        j = lax.broadcasted_iota(jnp.int32, (group, group), 1) // half
        mask = jnp.logical_and(i % 2 == 1, j == i - 1)
        for first in range(0, size, group):
            at = slice(first, first + group)
            w = w_ref[at, at]
            w_ref[at, at] = w - exact(w, exact(jnp.where(mask, a_ref[at, at], 0.0), w))
        half *= 2
    while half < size:
        for first in range(0, size, 2 * half):
            top = slice(first, first + half)
            low = slice(first + half, first + 2 * half)
            w_ref[low, top] = -exact(w_ref[low, low], exact(a_ref[low, top], w_ref[top, top]))
        half *= 2


def kernel(
    tri, rhs, out,
    grid, own, moved, inverse, solved, state,
    own_sem, rhs_send, rhs_recv, move_send, move_recv,
    grid_recv, source_send, pass_send,
    solved_send, solved_recv, solved_pass, out_send, out_recv,
):
    nb = own.shape[1]
    ncol = state.shape[2]
    sub = nb // 16
    part = nb // PIECES
    row = lax.axis_index("row")
    col = lax.axis_index("col")
    z, h = row // 2, row % 2
    x, low, q = col // 4, (col // 2) % 2, col % 2
    y = 2 * h + low
    first_row = 2 * z + q
    second_row = 14 - 2 * z + q

    def device(z_to, x_to, y_to, core):
        return {"row": 2 * z_to + y_to // 2, "col": 4 * x_to + 2 * (y_to % 2) + core}

    def remote(src, dst, send, recv, target):
        return pltpu.make_async_remote_copy(
            src_ref=src, dst_ref=dst, send_sem=send, recv_sem=recv,
            device_id=target, device_id_type=MESH,
        )

    here = device(z, x, y, q)

    loads = [
        pltpu.make_async_copy(tri.at[pl.ds(j * nb, nb), :], own.at[j], own_sem.at[j])
        for j in range(2)
    ]
    for load in loads:
        load.start()

    def rhs_copy(j, c_to):
        x_to, low_to, h_to = c_to // 4, (c_to // 2) % 2, c_to % 2
        src = rhs.at[pl.ds(j * sub, sub), pl.ds(pl.multiple_of(c_to * ncol, ncol), ncol)]
        dst = state.at[j, pl.ds(pl.multiple_of(col * sub, sub), sub), :]
        z_to = z if j == 0 else 3 - z
        return remote(
            src, dst, rhs_send.at[j, c_to], rhs_recv.at[j],
            device(z_to, x_to, 2 * h_to + low_to, h),
        ), pltpu.make_async_copy(src, dst, rhs_recv.at[j])

    chip = 4 * x + 2 * low + h

    def rhs_stays(j, c_to):
        return jnp.logical_and(j == 0, jnp.logical_and(c_to == chip, q == h))

    for j in range(2):

        @pl.loop(0, 16)
        def _(step, j=j):
            c_to = (step + chip) % 16
            away, home = rhs_copy(j, c_to)
            stays = rhs_stays(j, c_to)

            @pl.when(stays)
            def _():
                home.start()

            @pl.when(jnp.logical_not(stays))
            def _():
                away.start()

    for load in loads:
        load.wait()

    is_diag = col % 8 == row
    diag_slot = col // 8

    move = remote(own.at[1], moved, move_send, move_recv, device(3 - z, x, y, q))
    move_needed = col <= 8 + row
    moved_needed = col <= 14 - 2 * z + h
    early = jnp.logical_and(move_needed, jnp.logical_not(jnp.logical_and(is_diag, diag_slot == 1)))
    late = jnp.logical_and(is_diag, diag_slot == 1)

    @pl.when(early)
    def _():
        move.start()


    def sends(piece, k, dx, dy):
        par = (k // 2 + k) % 2
        first_is_y = piece % 2 == 0
        da, db = (dy, dx) if first_is_y else (dx, dy)
        on_line = db == 0
        first_plus = jnp.logical_and(on_line, jnp.logical_or(da == 0, jnp.logical_and(da == 1, par == 0)))
        first_minus = jnp.logical_and(on_line, jnp.logical_or(da == 0, jnp.logical_and(da == 3, par == 1)))
        second_plus = jnp.logical_or(on_line, jnp.logical_and(db == 1, par == 0))
        second_minus = jnp.logical_or(on_line, jnp.logical_and(db == 3, par == 1))
        if first_is_y:
            return second_plus, second_minus, first_plus, first_minus
        return first_plus, first_minus, second_plus, second_minus

    def neighbour(way, core):
        if way == 0:
            return device(z, (x + 1) % 4, y, core)
        if way == 1:
            return device(z, (x + 3) % 4, y, core)
        if way == 2:
            return device(z, x, (y + 1) % 4, core)
        return device(z, x, (y + 3) % 4, core)

    def rows_of(piece):
        return pl.ds(piece * part, part)

    def source_copies(j):
        src = own.at[0] if j == 0 else moved
        for piece in range(PIECES):
            for way in range(5):
                target = neighbour(way, h) if way < 4 else device(z, x, y, h)
                yield way, remote(
                    src.at[rows_of(piece), :],
                    grid.at[j, col, rows_of(piece), :],
                    source_send.at[j, piece, way],
                    grid_recv.at[j, col, piece],
                    target,
                )

    def source(j):
        for way, copy in source_copies(j):
            if way < 4:
                copy.start()
            else:

                @pl.when(q != h)
                def _(copy=copy):
                    copy.start()

        @pl.when(q == h)
        def _():
            grid[j, col] = own[0] if j == 0 else moved[...]

    def source_wait(j):
        for way, copy in source_copies(j):
            if way < 4:
                copy.wait_send()
            else:

                @pl.when(q != h)
                def _(copy=copy):
                    copy.wait_send()

    source_first = col <= row

    @pl.when(jnp.logical_and(source_first, jnp.logical_not(is_diag)))
    def _():
        source(0)

    @pl.when(is_diag)
    def _():
        invert(own.at[diag_slot], inverse)
        own[diag_slot] = inverse[...]

    @pl.when(late)
    def _():
        move.start()

    @pl.when(jnp.logical_and(source_first, is_diag))
    def _():
        source(0)

    def passing(j, k, do):
        dx = (x - k // 4 + 4) % 4
        dy = (y - 2 * q - (k // 2) % 2 + 4) % 4
        at_source = jnp.logical_and(dx == 0, dy == 0)
        is_source = jnp.logical_and(at_source, k % 2 == q)
        for piece in range(PIECES):
            spot = grid.at[j, k, rows_of(piece), :]
            copies = [
                remote(spot, spot, pass_send.at[j, k, piece, way], grid_recv.at[j, k, piece], neighbour(way, q))
                for way in range(4)
            ]
            flags = sends(piece, k, dx, dy)
            if do == "pass":

                @pl.when(jnp.logical_not(is_source))
                def _(copies=copies):
                    copies[0].wait_recv()

            for way in range(4):

                @pl.when(jnp.logical_and(flags[way], jnp.logical_not(at_source)))
                def _(copy=copies[way]):
                    if do == "pass":
                        copy.start()
                    else:
                        copy.wait_send()

    @pl.loop(0, first_row + 1)
    def _(k):
        passing(0, k, "pass")

    @pl.when(moved_needed)
    def _():
        move.wait_recv()
        source(1)

    @pl.loop(0, second_row + 1)
    def _(k):
        passing(1, k, "pass")

    for j in range(2):
        remote(state.at[j], state.at[j], rhs_send.at[j, 0], rhs_recv.at[j], here).wait_recv()

    def owner_z(k):
        return jnp.where(k < 8, k // 2, 7 - k // 2)

    def wanted(k, z_to):
        return jnp.logical_or(k < 8, z_to < owner_z(k))

    def solved_copies(k):
        spot = solved.at[k]
        partner_wants = jnp.logical_or(k % 2 == 0, k < 8)
        result = []
        for way in range(4):
            if way == 0:
                target, flag = device(z, x, y, 1 - q), partner_wants
            else:
                z_to = (z + (1, 3, 2)[way - 1]) % 4
                target, flag = device(z_to, x, y, 0), wanted(k, z_to)
            result.append((flag, remote(spot, spot, solved_send.at[k, way], solved_recv.at[k], target)))
        return result

    def out_copy(k):
        spot = out.at[pl.ds(pl.multiple_of((k // 8) * nb, nb), nb), :]
        stays = jnp.logical_and(k < 8, h == q)
        target = device((k % 8) // 2, x, 2 * q + low, h)
        away = remote(solved.at[k], spot, out_send.at[k // 8], out_recv.at[k // 8], target)
        home = pltpu.make_async_copy(solved.at[k], spot, out_recv.at[k // 8])
        return stays, away, home

    def is_owner(k):
        return jnp.logical_and(owner_z(k) == z, k % 2 == q)

    def pass_to_partner(k):
        spot = solved.at[k]
        flag = jnp.logical_and(q == 0, jnp.logical_and(owner_z(k) != z, wanted(k, z)))
        return flag, remote(spot, spot, solved_pass.at[k], solved_recv.at[k], device(z, x, y, 1))

    def gets(k):
        same_chip = owner_z(k) == z
        other_core = jnp.logical_and(same_chip, jnp.logical_and(k % 2 != q, jnp.logical_or(k % 2 == 0, k < 8)))
        return jnp.logical_or(other_core, jnp.logical_and(jnp.logical_not(same_chip), wanted(k, z)))

    @pl.loop(0, 16)
    def _(k):
        slot = k // 8

        @pl.when(is_owner(k))
        def _():
            solved[k] = product(grid[slot, k], state[slot])
            for flag, copy in solved_copies(k):

                @pl.when(flag)
                def _(copy=copy):
                    copy.start()

            stays, away, home = out_copy(k)

            @pl.when(stays)
            def _():
                home.start()

            @pl.when(jnp.logical_not(stays))
            def _():
                away.start()

        @pl.when(gets(k))
        def _():
            spot = solved.at[k]
            remote(spot, spot, solved_pass.at[k], solved_recv.at[k], here).wait_recv()
            flag, copy = pass_to_partner(k)

            @pl.when(flag)
            def _():
                copy.start()

        @pl.when(k < first_row)
        def _():
            state[0] = state[0] - product(grid[0, k], solved[k])

        @pl.when(k < second_row)
        def _():
            state[1] = state[1] - product(grid[1, k], solved[k])

    @pl.loop(0, 16)
    def _(k):
        @pl.when(is_owner(k))
        def _():
            for flag, copy in solved_copies(k):

                @pl.when(flag)
                def _(copy=copy):
                    copy.wait_send()

            stays, away, _ = out_copy(k)

            @pl.when(jnp.logical_not(stays))
            def _():
                away.wait_send()

        flag, copy = pass_to_partner(k)

        @pl.when(flag)
        def _():
            copy.wait_send()

        @pl.when(k <= first_row)
        def _():
            passing(0, k, "done")

        @pl.when(k <= second_row)
        def _():
            passing(1, k, "done")

    @pl.when(source_first)
    def _():
        source_wait(0)

    @pl.when(moved_needed)
    def _():
        source_wait(1)

    @pl.when(move_needed)
    def _():
        move.wait_send()

    for j in range(2):

        @pl.loop(0, 16)
        def _(c_to, j=j):
            away, _ = rhs_copy(j, c_to)

            @pl.when(jnp.logical_not(rhs_stays(j, c_to)))
            def _():
                away.wait_send()

        spot = out.at[pl.ds(j * nb, nb), :]
        remote(solved.at[0], spot, out_send.at[j], out_recv.at[j], here).wait_recv()


def on_device(tri, rhs):
    nb = tri.shape[1]
    ncol = rhs.shape[1] // 16
    dma = pltpu.SemaphoreType.DMA
    return pl.pallas_call(
        kernel,
        out_shape=jax.ShapeDtypeStruct((2 * nb, ncol), F32),
        in_specs=[pl.BlockSpec(memory_space=pl.ANY)] * 2,
        out_specs=pl.BlockSpec(memory_space=pl.ANY),
        scratch_shapes=[
            pltpu.VMEM((2, 16, nb, nb), F32),
            pltpu.VMEM((2, nb, nb), F32),
            pltpu.VMEM((nb, nb), F32),
            pltpu.VMEM((nb, nb), F32),
            pltpu.VMEM((16, nb, ncol), F32),
            pltpu.VMEM((2, nb, ncol), F32),
            dma((2,)),
            dma((2, 16)),
            dma((2,)),
            dma,
            dma,
            dma((2, 16, PIECES)),
            dma((2, PIECES, 5)),
            dma((2, 16, PIECES, 4)),
            dma((16, 4)),
            dma((16,)),
            dma((16,)),
            dma((2,)),
            dma((2,)),
        ],
        compiler_params=pltpu.CompilerParams(
            has_side_effects=True, vmem_limit_bytes=60 * 1024 * 1024
        ),
    )(tri, rhs)


def solution(mesh):
    return jax.shard_map(
        on_device,
        mesh=mesh,
        in_specs=(P("row", "col"), P(("row", "col"), None)),
        out_specs=P("row", "col"),
        check_vma=False,
    )
```

```python
import functools

import jax
import jax.numpy as jnp
from jax import lax
from jax.experimental import pallas as pl
from jax.experimental.pallas import tpu as pltpu
from jax.sharding import PartitionSpec as P

MESH = pl.DeviceIdType.MESH
F32 = jnp.float32
PIECES = 4
FIRST_Y = (True, False, True, False)
HIGH = lax.Precision.HIGHEST


def split(a):
    top = a.astype(jnp.bfloat16)
    return top, (a - top.astype(F32)).astype(jnp.bfloat16)


def product(a, b):
    a_top, a_rest = split(a)
    b_top, b_rest = split(b)
    dot = functools.partial(jnp.dot, preferred_element_type=F32)
    return dot(a_top, b_top) + (dot(a_top, b_rest) + dot(a_rest, b_top))


def exact(a, b):
    return jnp.dot(a, b, precision=HIGH, preferred_element_type=F32)


def invert(a_ref, w_ref):
    size = a_ref.shape[0]
    base = min(32, size)
    group = min(128, size)
    w_ref[...] = jnp.zeros_like(w_ref)
    eye = (
        lax.broadcasted_iota(jnp.int32, (base, base), 0)
        == lax.broadcasted_iota(jnp.int32, (base, base), 1)
    )
    for first in range(0, size, group):
        spots = list(range(first, first + group, base))
        scaled, scales, solved = [], [], []
        for spot in spots:
            a = a_ref[spot : spot + base, spot : spot + base]
            diag = jnp.where(eye, a, 0.0)
            inv_col = 1.0 / jnp.sum(diag, axis=1, keepdims=True)
            scales.append(1.0 / jnp.sum(diag, axis=0, keepdims=True))
            scaled.append(jnp.where(eye, 0.0, a * inv_col))
            solved.append(jnp.where(eye, jnp.ones((), F32), jnp.zeros((), F32)))
        for i in range(base - 1):
            for n in range(len(spots)):
                solved[n] = solved[n] - scaled[n][:, i : i + 1] * solved[n][i : i + 1, :]
        for n, spot in enumerate(spots):
            w_ref[spot : spot + base, spot : spot + base] = solved[n] * scales[n]
    half = base
    while half < group:
        i = lax.broadcasted_iota(jnp.int32, (group, group), 0) // half
        j = lax.broadcasted_iota(jnp.int32, (group, group), 1) // half
        mask = jnp.logical_and(i % 2 == 1, j == i - 1)
        for first in range(0, size, group):
            at = slice(first, first + group)
            w = w_ref[at, at]
            w_ref[at, at] = w - exact(w, exact(jnp.where(mask, a_ref[at, at], 0.0), w))
        half *= 2
    while half < size:
        for first in range(0, size, 2 * half):
            top = slice(first, first + half)
            low = slice(first + half, first + 2 * half)
            w_ref[low, top] = -exact(w_ref[low, low], exact(a_ref[low, top], w_ref[top, top]))
        half *= 2


def kernel(
    tri, rhs, out,
    grid, own, inverse, solved, state,
    own_sem, rhs_send, rhs_recv,
    grid_recv, source_send, pass_send,
    solved_send, solved_recv, solved_pass, out_send, out_recv,
):
    nb = own.shape[1]
    ncol = state.shape[2]
    sub = nb // 16
    part = nb // PIECES
    row = lax.axis_index("row")
    col = lax.axis_index("col")
    z, h = row // 2, row % 2
    x, low, q = col // 4, (col // 2) % 2, col % 2
    y = 2 * h + low
    first_row = 2 * z + q
    second_row = 8 + first_row

    def device(z_to, x_to, y_to, core):
        return {"row": 2 * z_to + y_to // 2, "col": 4 * x_to + 2 * (y_to % 2) + core}

    def remote(src, dst, send, recv, target):
        return pltpu.make_async_remote_copy(
            src_ref=src, dst_ref=dst, send_sem=send, recv_sem=recv,
            device_id=target, device_id_type=MESH,
        )

    here = device(z, x, y, q)

    barrier = pltpu.get_barrier_semaphore()

    def greet(target):
        pl.semaphore_signal(barrier, inc=1, device_id=target, device_id_type=MESH)

    @pl.loop(1, 32)
    def _(step):
        other = (16 * h + col + step) % 32
        greet({"row": 2 * z + other // 16, "col": other % 16})

    for step in range(1, 4):
        for core in range(2):
            greet(device((z + step) % 4, x, y, core))

    loads = [
        pltpu.make_async_copy(tri.at[pl.ds(j * nb, nb), :], own.at[j], own_sem.at[j])
        for j in range(2)
    ]
    for load in loads:
        load.start()

    pl.semaphore_wait(barrier, 37)

    def rhs_copy(j, c_to):
        x_to, low_to, h_to = c_to // 4, (c_to // 2) % 2, c_to % 2
        src = rhs.at[pl.ds(j * sub, sub), pl.ds(pl.multiple_of(c_to * ncol, ncol), ncol)]
        dst = state.at[j, pl.ds(pl.multiple_of(col * sub, sub), sub), :]
        return remote(
            src, dst, rhs_send.at[j, c_to], rhs_recv.at[j],
            device(z, x_to, 2 * h_to + low_to, h),
        ), pltpu.make_async_copy(src, dst, rhs_recv.at[j])

    chip = 4 * x + 2 * low + h

    def rhs_stays(c_to):
        return jnp.logical_and(c_to == chip, q == h)

    for j in range(2):

        @pl.loop(0, 16)
        def _(step, j=j):
            c_to = (step + chip) % 16
            away, home = rhs_copy(j, c_to)
            stays = rhs_stays(c_to)

            @pl.when(stays)
            def _():
                home.start()

            @pl.when(jnp.logical_not(stays))
            def _():
                away.start()

    for load in loads:
        load.wait()

    is_diag = col % 8 == row
    diag_slot = col // 8

    def edges(piece, k, dx, dy):
        ways = {0: (dx, (k % 2)), 2: (dy, ((k + k // 2) % 2))}
        first = 2 if FIRST_Y[piece] else 0
        gap, par = ways[first]
        on_line = ways[2 - first][0] == 0
        flags = {
            first: on_line & ((gap == 0) | ((gap == 1) & (par == 0))),
            first + 1: on_line & ((gap == 0) | ((gap == 3) & (par == 1))),
        }
        gap, par = ways[2 - first]
        flags[2 - first] = (gap == 0) | ((gap == 1) & (par == 0))
        flags[3 - first] = (gap == 0) | ((gap == 3) & (par == 1))
        return flags

    def neighbour(way, core):
        if way == 0:
            return device(z, (x + 1) % 4, y, core)
        if way == 1:
            return device(z, (x + 3) % 4, y, core)
        if way == 2:
            return device(z, x, (y + 1) % 4, core)
        return device(z, x, (y + 3) % 4, core)

    def rows_of(piece):
        return pl.ds(piece * part, part)

    def source_copies(j):
        src = own.at[j]
        for piece in range(PIECES):
            for way in range(5):
                target = neighbour(way, h) if way < 4 else device(z, x, y, h)
                yield way, remote(
                    src.at[rows_of(piece), :],
                    grid.at[j, col, rows_of(piece), :],
                    source_send.at[j, piece, way],
                    grid_recv.at[j, col, piece],
                    target,
                )

    def source(j):
        for way, copy in source_copies(j):
            if way < 4:
                copy.start()
            else:

                @pl.when(q != h)
                def _(copy=copy):
                    copy.start()

        @pl.when(q == h)
        def _():
            grid[j, col] = own[j]

    def source_wait(j):
        for way, copy in source_copies(j):
            if way < 4:
                copy.wait_send()
            else:

                @pl.when(q != h)
                def _(copy=copy):
                    copy.wait_send()

    needed = (col <= row, col <= 8 + row)
    diag_first = is_diag & (diag_slot == 0)
    diag_second = is_diag & (diag_slot == 1)

    pl.when(needed[0] & jnp.logical_not(diag_first))(lambda: source(0))

    @pl.when(is_diag)
    def _():
        invert(own.at[diag_slot], inverse)
        own[diag_slot] = inverse[...]

    pl.when(diag_first)(lambda: source(0))
    pl.when(needed[1])(lambda: source(1))

    reach = (0, 1, 2, 1)
    offsets = sorted(((dx, dy) for dx in range(4) for dy in range(4)), key=lambda o: reach[o[0]] + reach[o[1]])

    def offset_of(n):
        dx = dy = jnp.int32(0)
        for i, (a, b) in enumerate(offsets):
            dx, dy = jnp.where(n == i, a, dx), jnp.where(n == i, b, dy)
        return dx, dy

    def number_of(dx, dy):
        n = jnp.int32(0)
        for i, (a, b) in enumerate(offsets):
            n = jnp.where((dx == a) & (dy == b), i, n)
        return n

    def passing(j, n, limit, do, after=None):
        dx, dy = offset_of(n)
        x_from, y_from = (x - dx + 4) % 4, (y - dy + 4) % 4
        away = n > 0
        for side in range(2):
            k = 4 * x_from + 2 * (y_from % 2) + side

            @pl.when((y_from // 2 == q) & (k <= limit))
            def _(k=k, side=side):
                for piece in range(PIECES):
                    spot = grid.at[j, k, rows_of(piece), :]

                    def copy(way, spot=spot, piece=piece):
                        return remote(spot, spot, pass_send.at[j, k, piece, way], grid_recv.at[j, k, piece], neighbour(way, q))

                    if do == "pass":
                        pl.when(away | (q != side))(lambda copy=copy: copy(0).wait_recv())
                    for way, flag in edges(piece, k, dx, dy).items():

                        @pl.when(flag & away)
                        def _(copy=copy, way=way):
                            if do == "pass":
                                copy(way).start()
                            else:
                                copy(way).wait_send()

                if after is not None:
                    after(k)

    @pl.loop(0, 16)
    def _(n):
        passing(0, n, first_row, "pass")

    for j in range(2):
        remote(state.at[j], state.at[j], rhs_send.at[j, 0], rhs_recv.at[j], here).wait_recv()

    def owner_z(k):
        return (k % 8) // 2

    def wanted(k, z_to):
        return (k < 8) | (z_to > owner_z(k))

    def solved_copies(k):
        spot = solved.at[k]
        partner_wants = jnp.logical_or(k % 2 == 0, k < 8)
        result = []
        for way in range(4):
            if way == 0:
                target, flag = device(z, x, y, 1 - q), partner_wants
            else:
                z_to = (z + (1, 3, 2)[way - 1]) % 4
                target, flag = device(z_to, x, y, 0), wanted(k, z_to)
            result.append((flag, remote(spot, spot, solved_send.at[k, way], solved_recv.at[k], target)))
        return result

    def out_copy(k):
        spot = out.at[pl.ds(pl.multiple_of((k // 8) * nb, nb), nb), :]
        stays = h == q
        target = device(z, x, 2 * q + low, h)
        away = remote(solved.at[k], spot, out_send.at[k // 8], out_recv.at[k // 8], target)
        home = pltpu.make_async_copy(solved.at[k], spot, out_recv.at[k // 8])
        return stays, away, home

    def is_owner(k):
        return jnp.logical_and(owner_z(k) == z, k % 2 == q)

    def pass_to_partner(k):
        spot = solved.at[k]
        flag = jnp.logical_and(q == 0, jnp.logical_and(owner_z(k) != z, wanted(k, z)))
        return flag, remote(spot, spot, solved_pass.at[k], solved_recv.at[k], device(z, x, y, 1))

    def gets(k):
        same_chip = owner_z(k) == z
        other_core = jnp.logical_and(same_chip, jnp.logical_and(k % 2 != q, jnp.logical_or(k % 2 == 0, k < 8)))
        return jnp.logical_or(other_core, jnp.logical_and(jnp.logical_not(same_chip), wanted(k, z)))

    def solve(k):
        slot = k // 8
        solved[k] = product(grid[slot, k], state[slot])
        for flag, copy in solved_copies(k):
            pl.when(flag)(copy.start)
        stays, away, home = out_copy(k)
        pl.when(stays)(home.start)
        pl.when(jnp.logical_not(stays))(away.start)

    def update(slot, k):
        state[slot] = state[slot] - product(grid[slot, k], solved[k])

    span = 7 + 2 * z

    def passed(k):
        return jnp.minimum((16 * k) // span, 16)

    @pl.loop(-1, 16)
    def _(k):
        @pl.when((k >= 0) & gets(k))
        def _():
            spot = solved.at[k]
            remote(spot, spot, solved_pass.at[k], solved_recv.at[k], here).wait_recv()
            flag, copy = pass_to_partner(k)
            pl.when(flag)(copy.start)

        k_y = 2 * q + (k // 2) % 2
        taken = number_of((x - k // 4 + 4) % 4, (y - k_y + 4) % 4) < passed(k)
        early = (k >= 0) & (k < first_row)
        late = (k >= 0) & (k < second_row) & taken
        near = (k + 1) // 8

        @pl.when(jnp.where(k < 7, early, late) & (k < 15))
        def _():
            update(near, k)

        pl.when(is_owner(k + 1) & (k < 15))(lambda: solve(k + 1))

        @pl.when((k < 7) & late)
        def _():
            update(1, k)

        @pl.when(k >= 0)
        def _():
            def after(column):
                pl.when((column <= k) & (column < second_row))(lambda: update(1, column))

            @pl.loop(passed(k), passed(k + 1))
            def _(n):
                passing(1, n, second_row, "pass", after)

    @pl.loop(0, 16)
    def _(k):
        @pl.when(is_owner(k))
        def _():
            for flag, copy in solved_copies(k):

                @pl.when(flag)
                def _(copy=copy):
                    copy.wait_send()

            stays, away, _ = out_copy(k)

            @pl.when(jnp.logical_not(stays))
            def _():
                away.wait_send()

        flag, copy = pass_to_partner(k)

        @pl.when(flag)
        def _():
            copy.wait_send()

    @pl.loop(0, 16)
    def _(n):
        passing(0, n, first_row, "done")
        passing(1, n, second_row, "done")

    for j in range(2):
        pl.when(needed[j])(lambda j=j: source_wait(j))

    for j in range(2):

        @pl.loop(0, 16)
        def _(c_to, j=j):
            away, _ = rhs_copy(j, c_to)

            @pl.when(jnp.logical_not(rhs_stays(c_to)))
            def _():
                away.wait_send()

        spot = out.at[pl.ds(j * nb, nb), :]
        remote(solved.at[0], spot, out_send.at[j], out_recv.at[j], here).wait_recv()


def on_device(tri, rhs):
    nb = tri.shape[1]
    ncol = rhs.shape[1] // 16
    dma = pltpu.SemaphoreType.DMA
    return pl.pallas_call(
        kernel,
        out_shape=jax.ShapeDtypeStruct((2 * nb, ncol), F32),
        in_specs=[pl.BlockSpec(memory_space=pl.ANY)] * 2,
        out_specs=pl.BlockSpec(memory_space=pl.ANY),
        scratch_shapes=[
            pltpu.VMEM((2, 16, nb, nb), F32),
            pltpu.VMEM((2, nb, nb), F32),
            pltpu.VMEM((nb, nb), F32),
            pltpu.VMEM((16, nb, ncol), F32),
            pltpu.VMEM((2, nb, ncol), F32),
            dma((2,)),
            dma((2, 16)),
            dma((2,)),
            dma((2, 16, PIECES)),
            dma((2, PIECES, 5)),
            dma((2, 16, PIECES, 4)),
            dma((16, 4)),
            dma((16,)),
            dma((16,)),
            dma((2,)),
            dma((2,)),
        ],
        compiler_params=pltpu.CompilerParams(
            collective_id=0, has_side_effects=True, vmem_limit_bytes=60 * 1024 * 1024
        ),
    )(tri, rhs)


def solution(mesh):
    return jax.shard_map(
        on_device,
        mesh=mesh,
        in_specs=(P("row", "col"), P(("row", "col"), None)),
        out_specs=P("row", "col"),
        check_vma=False,
    )
```

```python
import functools

import jax
import jax.numpy as jnp
from jax import lax
from jax.experimental import pallas as pl
from jax.experimental.pallas import tpu as pltpu
from jax.sharding import PartitionSpec as P

MESH = pl.DeviceIdType.MESH
F32 = jnp.float32
PIECES = 4
FIRST_Y = (True, False, True, False)
HIGH = lax.Precision.HIGHEST


def split(a):
    top = a.astype(jnp.bfloat16)
    return top, (a - top.astype(F32)).astype(jnp.bfloat16)


def product(a, b):
    a_top, a_rest = split(a)
    b_top, b_rest = split(b)
    dot = functools.partial(jnp.dot, preferred_element_type=F32)
    return dot(a_top, b_top) + (dot(a_top, b_rest) + dot(a_rest, b_top))


def exact(a, b):
    return jnp.dot(a, b, precision=HIGH, preferred_element_type=F32)


def invert(a_ref, w_ref):
    size = a_ref.shape[0]
    base = min(32, size)
    group = min(128, size)
    w_ref[...] = jnp.zeros_like(w_ref)
    eye = (
        lax.broadcasted_iota(jnp.int32, (base, base), 0)
        == lax.broadcasted_iota(jnp.int32, (base, base), 1)
    )
    for first in range(0, size, group):
        spots = list(range(first, first + group, base))
        scaled, scales, solved = [], [], []
        for spot in spots:
            a = a_ref[spot : spot + base, spot : spot + base]
            diag = jnp.where(eye, a, 0.0)
            inv_col = 1.0 / jnp.sum(diag, axis=1, keepdims=True)
            scales.append(1.0 / jnp.sum(diag, axis=0, keepdims=True))
            scaled.append(jnp.where(eye, 0.0, a * inv_col))
            solved.append(jnp.where(eye, jnp.ones((), F32), jnp.zeros((), F32)))
        for i in range(base - 1):
            for n in range(len(spots)):
                solved[n] = solved[n] - scaled[n][:, i : i + 1] * solved[n][i : i + 1, :]
        for n, spot in enumerate(spots):
            w_ref[spot : spot + base, spot : spot + base] = solved[n] * scales[n]
    half = base
    while half < group:
        i = lax.broadcasted_iota(jnp.int32, (group, group), 0) // half
        j = lax.broadcasted_iota(jnp.int32, (group, group), 1) // half
        mask = jnp.logical_and(i % 2 == 1, j == i - 1)
        for first in range(0, size, group):
            at = slice(first, first + group)
            w = w_ref[at, at]
            w_ref[at, at] = w - exact(w, exact(jnp.where(mask, a_ref[at, at], 0.0), w))
        half *= 2
    while half < size:
        for first in range(0, size, 2 * half):
            top = slice(first, first + half)
            low = slice(first + half, first + 2 * half)
            w_ref[low, top] = -exact(w_ref[low, low], exact(a_ref[low, top], w_ref[top, top]))
        half *= 2


def kernel(
    tri, rhs, out,
    grid, own, inverse, solved, state,
    own_sem, rhs_send, rhs_recv,
    grid_recv, source_send, pass_send,
    solved_send, solved_recv, solved_pass, out_send, out_recv,
):
    nb = own.shape[1]
    ncol = state.shape[2]
    sub = nb // 16
    part = nb // PIECES
    row = lax.axis_index("row")
    col = lax.axis_index("col")
    z, h = row // 2, row % 2
    x, low, q = col // 4, (col // 2) % 2, col % 2
    y = 2 * h + low
    first_row = 2 * z + q
    second_row = 8 + first_row

    def device(z_to, x_to, y_to, core):
        return {"row": 2 * z_to + y_to // 2, "col": 4 * x_to + 2 * (y_to % 2) + core}

    def remote(src, dst, send, recv, target):
        return pltpu.make_async_remote_copy(
            src_ref=src, dst_ref=dst, send_sem=send, recv_sem=recv,
            device_id=target, device_id_type=MESH,
        )

    here = device(z, x, y, q)

    barrier = pltpu.get_barrier_semaphore()

    def greet(target):
        pl.semaphore_signal(barrier, inc=1, device_id=target, device_id_type=MESH)

    @pl.loop(1, 32)
    def _(step):
        other = (16 * h + col + step) % 32
        greet({"row": 2 * z + other // 16, "col": other % 16})

    for step in range(1, 4):
        for core in range(2):
            greet(device((z + step) % 4, x, y, core))

    loads = [
        pltpu.make_async_copy(tri.at[pl.ds(j * nb, nb), :], own.at[j], own_sem.at[j])
        for j in range(2)
    ]
    for load in loads:
        load.start()

    pl.semaphore_wait(barrier, 37)

    def rhs_copy(j, c_to):
        x_to, low_to, h_to = c_to // 4, (c_to // 2) % 2, c_to % 2
        src = rhs.at[pl.ds(j * sub, sub), pl.ds(pl.multiple_of(c_to * ncol, ncol), ncol)]
        dst = state.at[j, pl.ds(pl.multiple_of(col * sub, sub), sub), :]
        return remote(
            src, dst, rhs_send.at[j, c_to], rhs_recv.at[j],
            device(z, x_to, 2 * h_to + low_to, h),
        ), pltpu.make_async_copy(src, dst, rhs_recv.at[j])

    chip = 4 * x + 2 * low + h

    def rhs_stays(c_to):
        return jnp.logical_and(c_to == chip, q == h)

    for j in range(2):

        @pl.loop(0, 16)
        def _(step, j=j):
            c_to = (step + chip) % 16
            away, home = rhs_copy(j, c_to)
            stays = rhs_stays(c_to)

            @pl.when(stays)
            def _():
                home.start()

            @pl.when(jnp.logical_not(stays))
            def _():
                away.start()

    for load in loads:
        load.wait()

    is_diag = col % 8 == row
    diag_slot = col // 8

    def edges(piece, k, dx, dy):
        ways = {0: (dx, ((k // 4 + 1) // 2 + 1 + (piece // 2) * k) % 2), 2: (dy, (k + k // 2) % 2)}
        first = 2 if FIRST_Y[piece] else 0
        gap, par = ways[first]
        on_line = ways[2 - first][0] == 0
        flags = {
            first: on_line & ((gap == 0) | ((gap == 1) & (par == 0))),
            first + 1: on_line & ((gap == 0) | ((gap == 3) & (par == 1))),
        }
        gap, par = ways[2 - first]
        flags[2 - first] = (gap == 0) | ((gap == 1) & (par == 0))
        flags[3 - first] = (gap == 0) | ((gap == 3) & (par == 1))
        return flags

    def neighbour(way, core):
        if way == 0:
            return device(z, (x + 1) % 4, y, core)
        if way == 1:
            return device(z, (x + 3) % 4, y, core)
        if way == 2:
            return device(z, x, (y + 1) % 4, core)
        return device(z, x, (y + 3) % 4, core)

    def rows_of(piece):
        return pl.ds(piece * part, part)

    def source_copies(j):
        src = own.at[j]
        for piece in range(PIECES):
            for way in range(5):
                target = neighbour(way, h) if way < 4 else device(z, x, y, h)
                yield way, remote(
                    src.at[rows_of(piece), :],
                    grid.at[j, col, rows_of(piece), :],
                    source_send.at[j, piece, way],
                    grid_recv.at[j, col, piece],
                    target,
                )

    def source(j):
        for way, copy in source_copies(j):
            if way < 4:
                copy.start()
            else:

                @pl.when(q != h)
                def _(copy=copy):
                    copy.start()

        @pl.when(q == h)
        def _():
            grid[j, col] = own[j]

    def source_wait(j):
        for way, copy in source_copies(j):
            if way < 4:
                copy.wait_send()
            else:

                @pl.when(q != h)
                def _(copy=copy):
                    copy.wait_send()

    needed = (col <= row, col <= 8 + row)
    diag_first = is_diag & (diag_slot == 0)
    diag_second = is_diag & (diag_slot == 1)

    pl.when(needed[0] & jnp.logical_not(diag_first))(lambda: source(0))

    @pl.when(is_diag)
    def _():
        invert(own.at[diag_slot], inverse)
        own[diag_slot] = inverse[...]

    pl.when(diag_first)(lambda: source(0))
    reach = (0, 1, 2, 1)
    offsets = sorted(((dx, dy) for dx in range(4) for dy in range(4)), key=lambda o: (reach[o[0]] + reach[o[1]], o[1], o[0]))

    def offset_of(n):
        dx = dy = jnp.int32(0)
        for i, (a, b) in enumerate(offsets):
            dx, dy = jnp.where(n == i, a, dx), jnp.where(n == i, b, dy)
        return dx, dy

    def number_of(dx, dy):
        n = jnp.int32(0)
        for i, (a, b) in enumerate(offsets):
            n = jnp.where((dx == a) & (dy == b), i, n)
        return n

    def passing(j, n, limit, do, after=None):
        dx, dy = offset_of(n)
        x_from, y_from = (x - dx + 4) % 4, (y - dy + 4) % 4
        away = n > 0
        for side in range(2):
            k = 4 * x_from + 2 * (y_from % 2) + side

            @pl.when((y_from // 2 == q) & (k <= limit))
            def _(k=k, side=side):
                for piece in range(PIECES):
                    spot = grid.at[j, k, rows_of(piece), :]

                    def copy(way, spot=spot, piece=piece):
                        return remote(spot, spot, pass_send.at[j, k, piece, way], grid_recv.at[j, k, piece], neighbour(way, q))

                    if do == "pass":
                        pl.when(away | (q != side))(lambda copy=copy: copy(0).wait_recv())
                    for way, flag in edges(piece, k, dx, dy).items():

                        @pl.when(flag & away)
                        def _(copy=copy, way=way):
                            if do == "pass":
                                copy(way).start()
                            else:
                                copy(way).wait_send()

                if after is not None:
                    after(k)

    ahead = 8 * jnp.maximum(z - 1, 0) // (3 - 1)
    at_once = z > 1

    pl.when(at_once & needed[1])(lambda: source(1))

    @pl.loop(0, 16)
    def _(n):
        passing(0, n, first_row, "pass")

        @pl.loop((n * ahead) // 16, ((n + 1) * ahead) // 16)
        def _(m):
            passing(1, m, second_row, "pass")

    pl.when(jnp.logical_not(at_once) & needed[1])(lambda: source(1))

    for j in range(2):
        remote(state.at[j], state.at[j], rhs_send.at[j, 0], rhs_recv.at[j], here).wait_recv()

    def owner_z(k):
        return (k % 8) // 2

    def wanted(k, z_to):
        return (k < 8) | (z_to > owner_z(k))

    def solved_copies(k):
        spot = solved.at[k]
        partner_wants = jnp.logical_or(k % 2 == 0, k < 8)
        result = []
        for way in range(4):
            if way == 0:
                target, flag = device(z, x, y, 1 - q), partner_wants
            else:
                z_to = (z + (1, 3, 2)[way - 1]) % 4
                target, flag = device(z_to, x, y, 0), wanted(k, z_to)
            result.append((flag, remote(spot, spot, solved_send.at[k, way], solved_recv.at[k], target)))
        return result

    def out_copy(k):
        spot = out.at[pl.ds(pl.multiple_of((k // 8) * nb, nb), nb), :]
        stays = h == q
        target = device(z, x, 2 * q + low, h)
        away = remote(solved.at[k], spot, out_send.at[k // 8], out_recv.at[k // 8], target)
        home = pltpu.make_async_copy(solved.at[k], spot, out_recv.at[k // 8])
        return stays, away, home

    def is_owner(k):
        return jnp.logical_and(owner_z(k) == z, k % 2 == q)

    def pass_to_partner(k):
        spot = solved.at[k]
        flag = jnp.logical_and(q == 0, jnp.logical_and(owner_z(k) != z, wanted(k, z)))
        return flag, remote(spot, spot, solved_pass.at[k], solved_recv.at[k], device(z, x, y, 1))

    def gets(k):
        same_chip = owner_z(k) == z
        other_core = jnp.logical_and(same_chip, jnp.logical_and(k % 2 != q, jnp.logical_or(k % 2 == 0, k < 8)))
        return jnp.logical_or(other_core, jnp.logical_and(jnp.logical_not(same_chip), wanted(k, z)))

    def solve(k):
        slot = k // 8
        solved[k] = product(grid[slot, k], state[slot])
        for flag, copy in solved_copies(k):
            pl.when(flag)(copy.start)
        stays, away, home = out_copy(k)
        pl.when(stays)(home.start)
        pl.when(jnp.logical_not(stays))(away.start)

    def update(slot, k):
        state[slot] = state[slot] - product(grid[slot, k], solved[k])

    def passed(k):
        return jnp.where(k <= 2 * z, ahead, 16)

    @pl.loop(-1, 16)
    def _(k):
        @pl.when((k >= 0) & gets(k))
        def _():
            spot = solved.at[k]
            remote(spot, spot, solved_pass.at[k], solved_recv.at[k], here).wait_recv()
            flag, copy = pass_to_partner(k)
            pl.when(flag)(copy.start)

        k_y = 2 * q + (k // 2) % 2
        taken = number_of((x - k // 4 + 4) % 4, (y - k_y + 4) % 4) < passed(k)
        early = (k >= 0) & (k < first_row)
        late = (k >= 0) & (k < second_row) & taken
        near = (k + 1) // 8

        @pl.when(jnp.where(k < 7, early, late) & (k < 15))
        def _():
            update(near, k)

        pl.when(is_owner(k + 1) & (k < 15))(lambda: solve(k + 1))

        @pl.when((k < 7) & late)
        def _():
            update(1, k)

        @pl.when(k >= 0)
        def _():
            def after(column):
                pl.when((column <= k) & (column < second_row))(lambda: update(1, column))

            @pl.loop(passed(k), passed(k + 1))
            def _(n):
                passing(1, n, second_row, "pass", after)

    @pl.loop(0, 16)
    def _(k):
        @pl.when(is_owner(k))
        def _():
            for flag, copy in solved_copies(k):

                @pl.when(flag)
                def _(copy=copy):
                    copy.wait_send()

            stays, away, _ = out_copy(k)

            @pl.when(jnp.logical_not(stays))
            def _():
                away.wait_send()

        flag, copy = pass_to_partner(k)

        @pl.when(flag)
        def _():
            copy.wait_send()

    @pl.loop(0, 16)
    def _(n):
        passing(0, n, first_row, "done")
        passing(1, n, second_row, "done")

    for j in range(2):
        pl.when(needed[j])(lambda j=j: source_wait(j))

    for j in range(2):

        @pl.loop(0, 16)
        def _(c_to, j=j):
            away, _ = rhs_copy(j, c_to)

            @pl.when(jnp.logical_not(rhs_stays(c_to)))
            def _():
                away.wait_send()

        spot = out.at[pl.ds(j * nb, nb), :]
        remote(solved.at[0], spot, out_send.at[j], out_recv.at[j], here).wait_recv()


def on_device(tri, rhs):
    nb = tri.shape[1]
    ncol = rhs.shape[1] // 16
    dma = pltpu.SemaphoreType.DMA
    return pl.pallas_call(
        kernel,
        out_shape=jax.ShapeDtypeStruct((2 * nb, ncol), F32),
        in_specs=[pl.BlockSpec(memory_space=pl.ANY)] * 2,
        out_specs=pl.BlockSpec(memory_space=pl.ANY),
        scratch_shapes=[
            pltpu.VMEM((2, 16, nb, nb), F32),
            pltpu.VMEM((2, nb, nb), F32),
            pltpu.VMEM((nb, nb), F32),
            pltpu.VMEM((16, nb, ncol), F32),
            pltpu.VMEM((2, nb, ncol), F32),
            dma((2,)),
            dma((2, 16)),
            dma((2,)),
            dma((2, 16, PIECES)),
            dma((2, PIECES, 5)),
            dma((2, 16, PIECES, 4)),
            dma((16, 4)),
            dma((16,)),
            dma((16,)),
            dma((2,)),
            dma((2,)),
        ],
        compiler_params=pltpu.CompilerParams(
            collective_id=0, has_side_effects=True, vmem_limit_bytes=60 * 1024 * 1024
        ),
    )(tri, rhs)


def solution(mesh):
    return jax.shard_map(
        on_device,
        mesh=mesh,
        in_specs=(P("row", "col"), P(("row", "col"), None)),
        out_specs=P("row", "col"),
        check_vma=False,
    )
```

```python
import functools

import jax
import jax.numpy as jnp
from jax import lax
from jax.experimental import pallas as pl
from jax.experimental.pallas import tpu as pltpu
from jax.sharding import PartitionSpec as P

MESH = pl.DeviceIdType.MESH
F32 = jnp.float32
PIECES = 4
FIRST_Y = (True, False, True, False)
HIGH = lax.Precision.HIGHEST


def split(a):
    top = a.astype(jnp.bfloat16)
    return top, (a - top.astype(F32)).astype(jnp.bfloat16)


def product(a, b):
    a_top, a_rest = split(a)
    b_top, b_rest = split(b)
    dot = functools.partial(jnp.dot, preferred_element_type=F32)
    return dot(a_top, b_top) + (dot(a_top, b_rest) + dot(a_rest, b_top))


def exact(a, b):
    return jnp.dot(a, b, precision=HIGH, preferred_element_type=F32)


def invert(a_ref, w_ref):
    size = a_ref.shape[0]
    base = min(32, size)
    group = min(128, size)
    w_ref[...] = jnp.zeros_like(w_ref)
    eye = (
        lax.broadcasted_iota(jnp.int32, (base, base), 0)
        == lax.broadcasted_iota(jnp.int32, (base, base), 1)
    )
    for first in range(0, size, group):
        spots = list(range(first, first + group, base))
        scaled, scales, solved = [], [], []
        for spot in spots:
            a = a_ref[spot : spot + base, spot : spot + base]
            diag = jnp.where(eye, a, 0.0)
            inv_col = 1.0 / jnp.sum(diag, axis=1, keepdims=True)
            scales.append(1.0 / jnp.sum(diag, axis=0, keepdims=True))
            scaled.append(jnp.where(eye, 0.0, a * inv_col))
            solved.append(jnp.where(eye, jnp.ones((), F32), jnp.zeros((), F32)))
        for i in range(base - 1):
            for n in range(len(spots)):
                solved[n] = solved[n] - scaled[n][:, i : i + 1] * solved[n][i : i + 1, :]
        for n, spot in enumerate(spots):
            w_ref[spot : spot + base, spot : spot + base] = solved[n] * scales[n]
    half = base
    while half < group:
        i = lax.broadcasted_iota(jnp.int32, (group, group), 0) // half
        j = lax.broadcasted_iota(jnp.int32, (group, group), 1) // half
        mask = jnp.logical_and(i % 2 == 1, j == i - 1)
        for first in range(0, size, group):
            at = slice(first, first + group)
            w = w_ref[at, at]
            w_ref[at, at] = w - exact(w, exact(jnp.where(mask, a_ref[at, at], 0.0), w))
        half *= 2
    while half < size:
        for first in range(0, size, 2 * half):
            top = slice(first, first + half)
            low = slice(first + half, first + 2 * half)
            w_ref[low, top] = -exact(w_ref[low, low], exact(a_ref[low, top], w_ref[top, top]))
        half *= 2


def kernel(
    tri, rhs, out,
    grid, own, inverse, solved, state,
    own_sem, rhs_send, rhs_recv,
    grid_recv, source_send, pass_send,
    solved_send, solved_recv, solved_pass, out_send, out_recv,
):
    nb = own.shape[1]
    ncol = state.shape[2]
    sub = nb // 16
    part = nb // PIECES
    row = lax.axis_index("row")
    col = lax.axis_index("col")
    z, h = row // 2, row % 2
    x, low, q = col // 4, (col // 2) % 2, col % 2
    y = 2 * h + low
    first_row = 2 * z + q
    second_row = 8 + first_row

    def device(z_to, x_to, y_to, core):
        return {"row": 2 * z_to + y_to // 2, "col": 4 * x_to + 2 * (y_to % 2) + core}

    def remote(src, dst, send, recv, target):
        return pltpu.make_async_remote_copy(
            src_ref=src, dst_ref=dst, send_sem=send, recv_sem=recv,
            device_id=target, device_id_type=MESH,
        )

    here = device(z, x, y, q)

    barrier = pltpu.get_barrier_semaphore()

    def greet(target):
        pl.semaphore_signal(barrier, inc=1, device_id=target, device_id_type=MESH)

    @pl.loop(1, 32)
    def _(step):
        other = (16 * h + col + step) % 32
        greet({"row": 2 * z + other // 16, "col": other % 16})

    for step in range(1, 4):
        for core in range(2):
            greet(device((z + step) % 4, x, y, core))

    loads = [
        pltpu.make_async_copy(tri.at[pl.ds(j * nb, nb), :], own.at[j], own_sem.at[j])
        for j in range(2)
    ]
    for load in loads:
        load.start()

    pl.semaphore_wait(barrier, 37)

    def rhs_copy(j, c_to):
        x_to, low_to, h_to = c_to // 4, (c_to // 2) % 2, c_to % 2
        src = rhs.at[pl.ds(j * sub, sub), pl.ds(pl.multiple_of(c_to * ncol, ncol), ncol)]
        dst = state.at[j, pl.ds(pl.multiple_of(col * sub, sub), sub), :]
        return remote(
            src, dst, rhs_send.at[j, c_to], rhs_recv.at[j],
            device(z, x_to, 2 * h_to + low_to, h),
        ), pltpu.make_async_copy(src, dst, rhs_recv.at[j])

    chip = 4 * x + 2 * low + h

    def rhs_stays(c_to):
        return jnp.logical_and(c_to == chip, q == h)

    for j in range(2):

        @pl.loop(0, 16)
        def _(step, j=j):
            c_to = (step + chip) % 16
            away, home = rhs_copy(j, c_to)
            stays = rhs_stays(c_to)

            @pl.when(stays)
            def _():
                home.start()

            @pl.when(jnp.logical_not(stays))
            def _():
                away.start()

    for load in loads:
        load.wait()

    is_diag = col % 8 == row
    diag_slot = col // 8

    def edges(piece, k, dx, dy):
        ways = {0: (dx, k % 2), 2: (dy, (k + k // 2) % 2)}
        first = 2 if FIRST_Y[piece] else 0
        gap, par = ways[first]
        on_line = ways[2 - first][0] == 0
        flags = {
            first: on_line & ((gap == 0) | ((gap == 1) & (par == 0))),
            first + 1: on_line & ((gap == 0) | ((gap == 3) & (par == 1))),
        }
        gap, par = ways[2 - first]
        flags[2 - first] = (gap == 0) | ((gap == 1) & (par == 0))
        flags[3 - first] = (gap == 0) | ((gap == 3) & (par == 1))
        return flags

    def neighbour(way, core):
        if way == 0:
            return device(z, (x + 1) % 4, y, core)
        if way == 1:
            return device(z, (x + 3) % 4, y, core)
        if way == 2:
            return device(z, x, (y + 1) % 4, core)
        return device(z, x, (y + 3) % 4, core)

    def rows_of(piece):
        return pl.ds(piece * part, part)

    def shifts(j, piece):
        return (z >= 2) & (j == 0) & (piece >= PIECES // 2)

    def source_copies(j):
        src = own.at[j]
        for piece in range(PIECES):
            shifted = shifts(j, piece)
            for way in range(6):
                if way < 4:
                    target, flag = neighbour(way, h), jnp.logical_not(shifted)
                elif way == 4:
                    target, flag = device(z, x, y, h), jnp.logical_not(shifted) & (q != h)
                else:
                    target, flag = device(z, (x + 2) % 4, y, h), shifted
                yield flag, remote(
                    src.at[rows_of(piece), :],
                    grid.at[j, col, rows_of(piece), :],
                    source_send.at[j, piece, way],
                    grid_recv.at[j, col, piece],
                    target,
                )

    def source(j):
        for flag, copy in source_copies(j):
            pl.when(flag)(copy.start)

        for piece in range(PIECES):

            @pl.when((q == h) & jnp.logical_not(shifts(j, piece)))
            def _(piece=piece):
                grid[j, col, rows_of(piece), :] = own[j, rows_of(piece), :]

    def source_wait(j):
        for flag, copy in source_copies(j):
            pl.when(flag)(copy.wait_send)

    needed = (col <= row, col <= 8 + row)
    diag_first = is_diag & (diag_slot == 0)
    diag_second = is_diag & (diag_slot == 1)

    pl.when(needed[0] & jnp.logical_not(diag_first))(lambda: source(0))

    @pl.when(is_diag)
    def _():
        invert(own.at[diag_slot], inverse)
        own[diag_slot] = inverse[...]

    pl.when(diag_first)(lambda: source(0))
    reach = (0, 1, 2, 1)
    offsets = sorted(((dx, dy) for dx in range(4) for dy in range(4)), key=lambda o: (reach[o[0]] + reach[o[1]], o[1], o[0]))

    def offset_of(n):
        dx = dy = jnp.int32(0)
        for i, (a, b) in enumerate(offsets):
            dx, dy = jnp.where(n == i, a, dx), jnp.where(n == i, b, dy)
        return dx, dy

    def number_of(dx, dy):
        n = jnp.int32(0)
        for i, (a, b) in enumerate(offsets):
            n = jnp.where((dx == a) & (dy == b), i, n)
        return n

    def passing(j, n, limit, do, after=None):
        dx, dy = offset_of(n)
        x_from, y_from = (x - dx + 4) % 4, (y - dy + 4) % 4
        away = n > 0
        for side in range(2):
            k = 4 * x_from + 2 * (y_from % 2) + side
            for piece in range(PIECES):
                shifted = shifts(j, piece)
                k_piece = jnp.where(shifted, (k + 8) % 16, k)

                @pl.when((y_from // 2 == q) & (k_piece <= limit))
                def _(k=k, k_piece=k_piece, piece=piece, side=side, shifted=shifted):
                    spot = grid.at[j, k_piece, rows_of(piece), :]

                    def copy(way):
                        return remote(spot, spot, pass_send.at[j, k_piece, piece, way], grid_recv.at[j, k_piece, piece], neighbour(way, q))

                    if do == "pass":
                        pl.when(away | (q != side) | shifted)(lambda: copy(0).wait_recv())
                    for way, flag in edges(piece, k, dx, dy).items():

                        @pl.when(flag & (away | shifted))
                        def _(way=way):
                            if do == "pass":
                                copy(way).start()
                            else:
                                copy(way).wait_send()

            if after is not None:
                pl.when((y_from // 2 == q) & (k <= limit))(lambda k=k: after(k))

    ahead = 6 * jnp.maximum(z - 1, 0) // 2
    at_once = z > 1

    pl.when(at_once & needed[1])(lambda: source(1))

    @pl.loop(0, 16)
    def _(n):
        passing(0, n, first_row, "pass")

        @pl.loop((n * ahead) // 16, ((n + 1) * ahead) // 16)
        def _(m):
            passing(1, m, second_row, "pass")

    pl.when(jnp.logical_not(at_once) & needed[1])(lambda: source(1))

    for j in range(2):
        remote(state.at[j], state.at[j], rhs_send.at[j, 0], rhs_recv.at[j], here).wait_recv()

    def owner_z(k):
        return (k % 8) // 2

    def wanted(k, z_to):
        return (k < 8) | (z_to > owner_z(k))

    def solved_copies(k):
        spot = solved.at[k]
        partner_wants = jnp.logical_or(k % 2 == 0, k < 8)
        result = []
        for way in range(4):
            if way == 0:
                target, flag = device(z, x, y, 1 - q), partner_wants
            else:
                z_to = (z + (1, 3, 2)[way - 1]) % 4
                target, flag = device(z_to, x, y, 0), wanted(k, z_to)
            result.append((flag, remote(spot, spot, solved_send.at[k, way], solved_recv.at[k], target)))
        return result

    def out_copy(k):
        spot = out.at[pl.ds(pl.multiple_of((k // 8) * nb, nb), nb), :]
        stays = h == q
        target = device(z, x, 2 * q + low, h)
        away = remote(solved.at[k], spot, out_send.at[k // 8], out_recv.at[k // 8], target)
        home = pltpu.make_async_copy(solved.at[k], spot, out_recv.at[k // 8])
        return stays, away, home

    def is_owner(k):
        return jnp.logical_and(owner_z(k) == z, k % 2 == q)

    def pass_to_partner(k):
        spot = solved.at[k]
        flag = jnp.logical_and(q == 0, jnp.logical_and(owner_z(k) != z, wanted(k, z)))
        return flag, remote(spot, spot, solved_pass.at[k], solved_recv.at[k], device(z, x, y, 1))

    def gets(k):
        same_chip = owner_z(k) == z
        other_core = jnp.logical_and(same_chip, jnp.logical_and(k % 2 != q, jnp.logical_or(k % 2 == 0, k < 8)))
        return jnp.logical_or(other_core, jnp.logical_and(jnp.logical_not(same_chip), wanted(k, z)))

    def solve(k):
        slot = k // 8
        solved[k] = product(grid[slot, k], state[slot])
        for flag, copy in solved_copies(k):
            pl.when(flag)(copy.start)
        stays, away, home = out_copy(k)
        pl.when(stays)(home.start)
        pl.when(jnp.logical_not(stays))(away.start)

    def update(slot, k):
        state[slot] = state[slot] - product(grid[slot, k], solved[k])

    def passed(k):
        return jnp.where(k <= 2 * z, ahead, jnp.minimum(jnp.maximum(10 + k - 2 * z, ahead), 16))

    @pl.loop(-1, 16)
    def _(k):
        @pl.when((k >= 0) & gets(k))
        def _():
            spot = solved.at[k]
            remote(spot, spot, solved_pass.at[k], solved_recv.at[k], here).wait_recv()
            flag, copy = pass_to_partner(k)
            pl.when(flag)(copy.start)

        k_y = 2 * q + (k // 2) % 2
        taken = number_of((x - k // 4 + 4) % 4, (y - k_y + 4) % 4) < passed(k)
        early = (k >= 0) & (k < first_row)
        late = (k >= 0) & (k < second_row) & taken
        near = (k + 1) // 8

        @pl.when(jnp.where(k < 7, early, late) & (k < 15))
        def _():
            update(near, k)

        pl.when(is_owner(k + 1) & (k < 15))(lambda: solve(k + 1))

        @pl.when((k < 7) & late)
        def _():
            update(1, k)

        @pl.when(k >= 0)
        def _():
            def after(column):
                pl.when((column <= k) & (column < second_row))(lambda: update(1, column))

            @pl.loop(passed(k), passed(k + 1))
            def _(n):
                passing(1, n, second_row, "pass", after)

    @pl.loop(0, 16)
    def _(k):
        @pl.when(is_owner(k))
        def _():
            for flag, copy in solved_copies(k):

                @pl.when(flag)
                def _(copy=copy):
                    copy.wait_send()

            stays, away, _ = out_copy(k)

            @pl.when(jnp.logical_not(stays))
            def _():
                away.wait_send()

        flag, copy = pass_to_partner(k)

        @pl.when(flag)
        def _():
            copy.wait_send()

    @pl.loop(0, 16)
    def _(n):
        passing(0, n, first_row, "done")
        passing(1, n, second_row, "done")

    for j in range(2):
        pl.when(needed[j])(lambda j=j: source_wait(j))

    for j in range(2):

        @pl.loop(0, 16)
        def _(c_to, j=j):
            away, _ = rhs_copy(j, c_to)

            @pl.when(jnp.logical_not(rhs_stays(c_to)))
            def _():
                away.wait_send()

        spot = out.at[pl.ds(j * nb, nb), :]
        remote(solved.at[0], spot, out_send.at[j], out_recv.at[j], here).wait_recv()


def on_device(tri, rhs):
    nb = tri.shape[1]
    ncol = rhs.shape[1] // 16
    dma = pltpu.SemaphoreType.DMA
    return pl.pallas_call(
        kernel,
        out_shape=jax.ShapeDtypeStruct((2 * nb, ncol), F32),
        in_specs=[pl.BlockSpec(memory_space=pl.ANY)] * 2,
        out_specs=pl.BlockSpec(memory_space=pl.ANY),
        scratch_shapes=[
            pltpu.VMEM((2, 16, nb, nb), F32),
            pltpu.VMEM((2, nb, nb), F32),
            pltpu.VMEM((nb, nb), F32),
            pltpu.VMEM((16, nb, ncol), F32),
            pltpu.VMEM((2, nb, ncol), F32),
            dma((2,)),
            dma((2, 16)),
            dma((2,)),
            dma((2, 16, PIECES)),
            dma((2, PIECES, 6)),
            dma((2, 16, PIECES, 4)),
            dma((16, 4)),
            dma((16,)),
            dma((16,)),
            dma((2,)),
            dma((2,)),
        ],
        compiler_params=pltpu.CompilerParams(
            collective_id=0, has_side_effects=True, vmem_limit_bytes=60 * 1024 * 1024
        ),
    )(tri, rhs)


def solution(mesh):
    return jax.shard_map(
        on_device,
        mesh=mesh,
        in_specs=(P("row", "col"), P(("row", "col"), None)),
        out_specs=P("row", "col"),
        check_vma=False,
    )
```

```python
import functools

import jax
import jax.numpy as jnp
from jax import lax
from jax.experimental import pallas as pl
from jax.experimental.pallas import tpu as pltpu
from jax.sharding import PartitionSpec as P

MESH = pl.DeviceIdType.MESH
F32 = jnp.float32
PIECES = 4
FIRST_Y = (True, False, True, False)
HIGH = lax.Precision.HIGHEST


def split(a):
    top = a.astype(jnp.bfloat16)
    return top, (a - top.astype(F32)).astype(jnp.bfloat16)


def product(a, b):
    a_top, a_rest = split(a)
    b_top, b_rest = split(b)
    dot = functools.partial(jnp.dot, preferred_element_type=F32)
    return dot(a_top, b_top) + (dot(a_top, b_rest) + dot(a_rest, b_top))


def exact(a, b):
    return jnp.dot(a, b, precision=HIGH, preferred_element_type=F32)


def invert(a_ref, w_ref):
    size = a_ref.shape[0]
    base = min(32, size)
    group = min(128, size)
    w_ref[...] = jnp.zeros_like(w_ref)
    eye = (
        lax.broadcasted_iota(jnp.int32, (base, base), 0)
        == lax.broadcasted_iota(jnp.int32, (base, base), 1)
    )
    for first in range(0, size, group):
        spots = list(range(first, first + group, base))
        scaled, scales, solved = [], [], []
        for spot in spots:
            a = a_ref[spot : spot + base, spot : spot + base]
            diag = jnp.where(eye, a, 0.0)
            inv_col = 1.0 / jnp.sum(diag, axis=1, keepdims=True)
            scales.append(1.0 / jnp.sum(diag, axis=0, keepdims=True))
            scaled.append(jnp.where(eye, 0.0, a * inv_col))
            solved.append(jnp.where(eye, jnp.ones((), F32), jnp.zeros((), F32)))
        for i in range(base - 1):
            for n in range(len(spots)):
                solved[n] = solved[n] - scaled[n][:, i : i + 1] * solved[n][i : i + 1, :]
        for n, spot in enumerate(spots):
            w_ref[spot : spot + base, spot : spot + base] = solved[n] * scales[n]
    half = base
    while half < group:
        i = lax.broadcasted_iota(jnp.int32, (group, group), 0) // half
        j = lax.broadcasted_iota(jnp.int32, (group, group), 1) // half
        mask = jnp.logical_and(i % 2 == 1, j == i - 1)
        for first in range(0, size, group):
            at = slice(first, first + group)
            w = w_ref[at, at]
            w_ref[at, at] = w - exact(w, exact(jnp.where(mask, a_ref[at, at], 0.0), w))
        half *= 2
    while half < size:
        for first in range(0, size, 2 * half):
            top = slice(first, first + half)
            low = slice(first + half, first + 2 * half)
            w_ref[low, top] = -exact(w_ref[low, low], exact(a_ref[low, top], w_ref[top, top]))
        half *= 2


def kernel(
    tri, rhs, out,
    grid, own, inverse, solved, state,
    own_sem, rhs_send, rhs_recv,
    grid_recv, source_send, pass_send,
    solved_send, solved_recv, solved_pass, out_send, out_recv,
):
    nb = own.shape[1]
    ncol = state.shape[2]
    sub = nb // 16
    part = nb // PIECES
    row = lax.axis_index("row")
    col = lax.axis_index("col")
    z, h = row // 2, row % 2
    x, low, q = col // 4, (col // 2) % 2, col % 2
    y = 2 * h + low
    first_row = 2 * z + q
    second_row = 8 + first_row

    def device(z_to, x_to, y_to, core):
        return {"row": 2 * z_to + y_to // 2, "col": 4 * x_to + 2 * (y_to % 2) + core}

    def remote(src, dst, send, recv, target):
        return pltpu.make_async_remote_copy(
            src_ref=src, dst_ref=dst, send_sem=send, recv_sem=recv,
            device_id=target, device_id_type=MESH,
        )

    here = device(z, x, y, q)

    barrier = pltpu.get_barrier_semaphore()

    def greet(target):
        pl.semaphore_signal(barrier, inc=1, device_id=target, device_id_type=MESH)

    @pl.loop(1, 32)
    def _(step):
        other = (16 * h + col + step) % 32
        greet({"row": 2 * z + other // 16, "col": other % 16})

    for step in range(1, 4):
        for core in range(2):
            greet(device((z + step) % 4, x, y, core))

    loads = [
        pltpu.make_async_copy(tri.at[pl.ds(j * nb, nb), :], own.at[j], own_sem.at[j])
        for j in range(2)
    ]
    for load in loads:
        load.start()

    pl.semaphore_wait(barrier, 37)

    def rhs_copy(j, c_to):
        x_to, low_to, h_to = c_to // 4, (c_to // 2) % 2, c_to % 2
        src = rhs.at[pl.ds(j * sub, sub), pl.ds(pl.multiple_of(c_to * ncol, ncol), ncol)]
        dst = state.at[j, pl.ds(pl.multiple_of(col * sub, sub), sub), :]
        return remote(
            src, dst, rhs_send.at[j, c_to], rhs_recv.at[j],
            device(z, x_to, 2 * h_to + low_to, h),
        ), pltpu.make_async_copy(src, dst, rhs_recv.at[j])

    chip = 4 * x + 2 * low + h

    def rhs_stays(c_to):
        return jnp.logical_and(c_to == chip, q == h)

    for j in range(2):

        @pl.loop(0, 16)
        def _(step, j=j):
            c_to = (step + chip) % 16
            away, home = rhs_copy(j, c_to)
            stays = rhs_stays(c_to)

            @pl.when(stays)
            def _():
                home.start()

            @pl.when(jnp.logical_not(stays))
            def _():
                away.start()

    for load in loads:
        load.wait()

    is_diag = col % 8 == row
    diag_slot = col // 8

    def edges(piece, k, dx, dy):
        ways = {0: (dx, k % 2), 2: (dy, (k + k // 2) % 2)}
        first = 2 if FIRST_Y[piece] else 0
        gap, par = ways[first]
        on_line = ways[2 - first][0] == 0
        flags = {
            first: on_line & ((gap == 0) | ((gap == 1) & (par == 0))),
            first + 1: on_line & ((gap == 0) | ((gap == 3) & (par == 1))),
        }
        gap, par = ways[2 - first]
        flags[2 - first] = (gap == 0) | ((gap == 1) & (par == 0))
        flags[3 - first] = (gap == 0) | ((gap == 3) & (par == 1))
        return flags

    def neighbour(way, core):
        if way == 0:
            return device(z, (x + 1) % 4, y, core)
        if way == 1:
            return device(z, (x + 3) % 4, y, core)
        if way == 2:
            return device(z, x, (y + 1) % 4, core)
        return device(z, x, (y + 3) % 4, core)

    def rows_of(piece):
        return pl.ds(piece * part, part)

    def shifts(j, piece):
        return (z >= 2) & (j == 0) & (piece >= PIECES // 2)

    def source_copies(j):
        src = own.at[j]
        for piece in range(PIECES):
            shifted = shifts(j, piece)
            for way in range(6):
                if way < 4:
                    target, flag = neighbour(way, h), jnp.logical_not(shifted)
                elif way == 4:
                    target, flag = device(z, x, y, h), jnp.logical_not(shifted) & (q != h)
                else:
                    target, flag = device(z, (x + 2) % 4, y, h), shifted
                yield flag, remote(
                    src.at[rows_of(piece), :],
                    grid.at[j, col, rows_of(piece), :],
                    source_send.at[j, piece, way],
                    grid_recv.at[j, col, piece],
                    target,
                )

    def source(j):
        for flag, copy in source_copies(j):
            pl.when(flag)(copy.start)

        for piece in range(PIECES):

            @pl.when((q == h) & jnp.logical_not(shifts(j, piece)))
            def _(piece=piece):
                grid[j, col, rows_of(piece), :] = own[j, rows_of(piece), :]

    def source_wait(j):
        for flag, copy in source_copies(j):
            pl.when(flag)(copy.wait_send)

    needed = (col <= row, col <= 8 + row)
    diag_first = is_diag & (diag_slot == 0)
    diag_second = is_diag & (diag_slot == 1)

    pl.when(needed[0] & jnp.logical_not(diag_first))(lambda: source(0))

    @pl.when(is_diag)
    def _():
        invert(own.at[diag_slot], inverse)
        own[diag_slot] = inverse[...]

    pl.when(diag_first)(lambda: source(0))
    reach = (0, 1, 2, 1)
    offsets = sorted(((dx, dy) for dx in range(4) for dy in range(4)), key=lambda o: (reach[o[0]] + 1.5 * reach[o[1]], o[1], o[0]))

    def offset_of(n):
        dx = dy = jnp.int32(0)
        for i, (a, b) in enumerate(offsets):
            dx, dy = jnp.where(n == i, a, dx), jnp.where(n == i, b, dy)
        return dx, dy

    def number_of(dx, dy):
        n = jnp.int32(0)
        for i, (a, b) in enumerate(offsets):
            n = jnp.where((dx == a) & (dy == b), i, n)
        return n

    def passing(j, n, limit, do, after=None):
        dx, dy = offset_of(n)
        x_from, y_from = (x - dx + 4) % 4, (y - dy + 4) % 4
        away = n > 0
        for side in range(2):
            k = 4 * x_from + 2 * (y_from % 2) + side
            for piece in range(PIECES):
                shifted = shifts(j, piece)
                k_piece = jnp.where(shifted, (k + 8) % 16, k)

                @pl.when((y_from // 2 == q) & (k_piece <= limit))
                def _(k=k, k_piece=k_piece, piece=piece, side=side, shifted=shifted):
                    spot = grid.at[j, k_piece, rows_of(piece), :]

                    def copy(way):
                        return remote(spot, spot, pass_send.at[j, k_piece, piece, way], grid_recv.at[j, k_piece, piece], neighbour(way, q))

                    if do == "pass":
                        pl.when(away | (q != side) | shifted)(lambda: copy(0).wait_recv())
                    for way, flag in edges(piece, k, dx, dy).items():

                        @pl.when(flag & (away | shifted))
                        def _(way=way):
                            if do == "pass":
                                copy(way).start()
                            else:
                                copy(way).wait_send()

            if after is not None:
                pl.when((y_from // 2 == q) & (k <= limit))(lambda k=k: after(k))

    ahead = 6 * jnp.maximum(z - 1, 0) // 2
    at_once = z > 1

    pl.when(at_once & needed[1])(lambda: source(1))

    @pl.loop(0, 16)
    def _(n):
        passing(0, n, first_row, "pass")

        @pl.loop((n * ahead) // 16, ((n + 1) * ahead) // 16)
        def _(m):
            passing(1, m, second_row, "pass")

    pl.when(jnp.logical_not(at_once) & needed[1])(lambda: source(1))

    for j in range(2):
        remote(state.at[j], state.at[j], rhs_send.at[j, 0], rhs_recv.at[j], here).wait_recv()

    def owner_z(k):
        return (k % 8) // 2

    def wanted(k, z_to):
        return (k < 8) | (z_to > owner_z(k))

    def solved_copies(k):
        spot = solved.at[k]
        partner_wants = jnp.logical_or(k % 2 == 0, k < 8)
        result = []
        for way in range(4):
            if way == 0:
                target, flag = device(z, x, y, 1 - q), partner_wants
            else:
                z_to = (z + (1, 3, 2)[way - 1]) % 4
                target, flag = device(z_to, x, y, 0), wanted(k, z_to)
            result.append((flag, remote(spot, spot, solved_send.at[k, way], solved_recv.at[k], target)))
        return result

    def out_copy(k):
        spot = out.at[pl.ds(pl.multiple_of((k // 8) * nb, nb), nb), :]
        stays = h == q
        target = device(z, x, 2 * q + low, h)
        away = remote(solved.at[k], spot, out_send.at[k // 8], out_recv.at[k // 8], target)
        home = pltpu.make_async_copy(solved.at[k], spot, out_recv.at[k // 8])
        return stays, away, home

    def is_owner(k):
        return jnp.logical_and(owner_z(k) == z, k % 2 == q)

    def pass_to_partner(k):
        spot = solved.at[k]
        flag = jnp.logical_and(q == 0, jnp.logical_and(owner_z(k) != z, wanted(k, z)))
        return flag, remote(spot, spot, solved_pass.at[k], solved_recv.at[k], device(z, x, y, 1))

    def gets(k):
        same_chip = owner_z(k) == z
        other_core = jnp.logical_and(same_chip, jnp.logical_and(k % 2 != q, jnp.logical_or(k % 2 == 0, k < 8)))
        return jnp.logical_or(other_core, jnp.logical_and(jnp.logical_not(same_chip), wanted(k, z)))

    def solve(k):
        slot = k // 8
        solved[k] = product(grid[slot, k], state[slot])
        for flag, copy in solved_copies(k):
            pl.when(flag)(copy.start)
        stays, away, home = out_copy(k)
        pl.when(stays)(home.start)
        pl.when(jnp.logical_not(stays))(away.start)

    def update(slot, k):
        state[slot] = state[slot] - product(grid[slot, k], solved[k])

    def passed(k):
        return jnp.where(k <= 2 * z, ahead, jnp.minimum(jnp.maximum(10 + k - 2 * z, ahead), 16))

    @pl.loop(-1, 16)
    def _(k):
        @pl.when((k >= 0) & gets(k))
        def _():
            spot = solved.at[k]
            remote(spot, spot, solved_pass.at[k], solved_recv.at[k], here).wait_recv()
            flag, copy = pass_to_partner(k)
            pl.when(flag)(copy.start)

        k_y = 2 * q + (k // 2) % 2
        taken = number_of((x - k // 4 + 4) % 4, (y - k_y + 4) % 4) < passed(k)
        early = (k >= 0) & (k < first_row)
        late = (k >= 0) & (k < second_row) & taken
        near = (k + 1) // 8

        @pl.when(jnp.where(k < 7, early, late) & (k < 15))
        def _():
            update(near, k)

        pl.when(is_owner(k + 1) & (k < 15))(lambda: solve(k + 1))

        @pl.when((k < 7) & late)
        def _():
            update(1, k)

        @pl.when(k >= 0)
        def _():
            def after(column):
                pl.when((column <= k) & (column < second_row))(lambda: update(1, column))

            @pl.loop(passed(k), passed(k + 1))
            def _(n):
                passing(1, n, second_row, "pass", after)

    @pl.loop(0, 16)
    def _(k):
        @pl.when(is_owner(k))
        def _():
            for flag, copy in solved_copies(k):

                @pl.when(flag)
                def _(copy=copy):
                    copy.wait_send()

            stays, away, _ = out_copy(k)

            @pl.when(jnp.logical_not(stays))
            def _():
                away.wait_send()

        flag, copy = pass_to_partner(k)

        @pl.when(flag)
        def _():
            copy.wait_send()

    @pl.loop(0, 16)
    def _(n):
        passing(0, n, first_row, "done")
        passing(1, n, second_row, "done")

    for j in range(2):
        pl.when(needed[j])(lambda j=j: source_wait(j))

    for j in range(2):

        @pl.loop(0, 16)
        def _(c_to, j=j):
            away, _ = rhs_copy(j, c_to)

            @pl.when(jnp.logical_not(rhs_stays(c_to)))
            def _():
                away.wait_send()

        spot = out.at[pl.ds(j * nb, nb), :]
        remote(solved.at[0], spot, out_send.at[j], out_recv.at[j], here).wait_recv()


def on_device(tri, rhs):
    nb = tri.shape[1]
    ncol = rhs.shape[1] // 16
    dma = pltpu.SemaphoreType.DMA
    return pl.pallas_call(
        kernel,
        out_shape=jax.ShapeDtypeStruct((2 * nb, ncol), F32),
        in_specs=[pl.BlockSpec(memory_space=pl.ANY)] * 2,
        out_specs=pl.BlockSpec(memory_space=pl.ANY),
        scratch_shapes=[
            pltpu.VMEM((2, 16, nb, nb), F32),
            pltpu.VMEM((2, nb, nb), F32),
            pltpu.VMEM((nb, nb), F32),
            pltpu.VMEM((16, nb, ncol), F32),
            pltpu.VMEM((2, nb, ncol), F32),
            dma((2,)),
            dma((2, 16)),
            dma((2,)),
            dma((2, 16, PIECES)),
            dma((2, PIECES, 6)),
            dma((2, 16, PIECES, 4)),
            dma((16, 4)),
            dma((16,)),
            dma((16,)),
            dma((2,)),
            dma((2,)),
        ],
        compiler_params=pltpu.CompilerParams(
            collective_id=0, has_side_effects=True, vmem_limit_bytes=60 * 1024 * 1024
        ),
    )(tri, rhs)


def solution(mesh):
    return jax.shard_map(
        on_device,
        mesh=mesh,
        in_specs=(P("row", "col"), P(("row", "col"), None)),
        out_specs=P("row", "col"),
        check_vma=False,
    )
```

```python
import functools

import jax
import jax.numpy as jnp
from jax import lax
from jax.experimental import pallas as pl
from jax.experimental.pallas import tpu as pltpu
from jax.sharding import PartitionSpec as P

MESH = pl.DeviceIdType.MESH
F32 = jnp.float32
PIECES = 4
FIRST_Y = (True, False, True, False)
HIGH = lax.Precision.HIGHEST


def split(a):
    top = a.astype(jnp.bfloat16)
    return top, (a - top.astype(F32)).astype(jnp.bfloat16)


def product(a, b):
    a_top, a_rest = split(a)
    b_top, b_rest = split(b)
    dot = functools.partial(jnp.dot, preferred_element_type=F32)
    return dot(a_top, b_top) + (dot(a_top, b_rest) + dot(a_rest, b_top))


def exact(a, b):
    return jnp.dot(a, b, precision=HIGH, preferred_element_type=F32)


def invert(a_ref, w_ref):
    size = a_ref.shape[0]
    base = min(32, size)
    group = min(128, size)
    w_ref[...] = jnp.zeros_like(w_ref)
    eye = (
        lax.broadcasted_iota(jnp.int32, (base, base), 0)
        == lax.broadcasted_iota(jnp.int32, (base, base), 1)
    )
    for first in range(0, size, group):
        spots = list(range(first, first + group, base))
        scaled, scales, solved = [], [], []
        for spot in spots:
            a = a_ref[spot : spot + base, spot : spot + base]
            diag = jnp.where(eye, a, 0.0)
            inv_col = 1.0 / jnp.sum(diag, axis=1, keepdims=True)
            scales.append(1.0 / jnp.sum(diag, axis=0, keepdims=True))
            scaled.append(jnp.where(eye, 0.0, a * inv_col))
            solved.append(jnp.where(eye, jnp.ones((), F32), jnp.zeros((), F32)))
        for i in range(base - 1):
            for n in range(len(spots)):
                solved[n] = solved[n] - scaled[n][:, i : i + 1] * solved[n][i : i + 1, :]
        for n, spot in enumerate(spots):
            w_ref[spot : spot + base, spot : spot + base] = solved[n] * scales[n]
    half = base
    while half < group:
        i = lax.broadcasted_iota(jnp.int32, (group, group), 0) // half
        j = lax.broadcasted_iota(jnp.int32, (group, group), 1) // half
        mask = jnp.logical_and(i % 2 == 1, j == i - 1)
        for first in range(0, size, group):
            at = slice(first, first + group)
            w = w_ref[at, at]
            w_ref[at, at] = w - exact(w, exact(jnp.where(mask, a_ref[at, at], 0.0), w))
        half *= 2
    while half < size:
        for first in range(0, size, 2 * half):
            top = slice(first, first + half)
            low = slice(first + half, first + 2 * half)
            w_ref[low, top] = -exact(w_ref[low, low], exact(a_ref[low, top], w_ref[top, top]))
        half *= 2


def kernel(
    tri, rhs, out,
    grid, own, inverse, solved, state,
    own_sem, rhs_send, rhs_recv,
    grid_recv, source_send, pass_send,
    solved_send, solved_recv, solved_pass, out_send, out_recv,
):
    nb = own.shape[1]
    ncol = state.shape[2]
    sub = nb // 16
    part = nb // PIECES
    row = lax.axis_index("row")
    col = lax.axis_index("col")
    z, h = row // 2, row % 2
    x, low, q = col // 4, (col // 2) % 2, col % 2
    y = 2 * h + low
    first_row = 2 * z + q
    second_row = 8 + first_row

    def device(z_to, x_to, y_to, core):
        return {"row": 2 * z_to + y_to // 2, "col": 4 * x_to + 2 * (y_to % 2) + core}

    def remote(src, dst, send, recv, target):
        return pltpu.make_async_remote_copy(
            src_ref=src, dst_ref=dst, send_sem=send, recv_sem=recv,
            device_id=target, device_id_type=MESH,
        )

    here = device(z, x, y, q)

    barrier = pltpu.get_barrier_semaphore()

    def greet(target):
        pl.semaphore_signal(barrier, inc=1, device_id=target, device_id_type=MESH)

    @pl.loop(1, 32)
    def _(step):
        other = (16 * h + col + step) % 32
        greet({"row": 2 * z + other // 16, "col": other % 16})

    for step in range(1, 4):
        for core in range(2):
            greet(device((z + step) % 4, x, y, core))

    loads = [
        pltpu.make_async_copy(tri.at[pl.ds(j * nb, nb), :], own.at[j], own_sem.at[j])
        for j in range(2)
    ]
    for load in loads:
        load.start()

    pl.semaphore_wait(barrier, 37)

    def rhs_copy(j, c_to):
        x_to, low_to, h_to = c_to // 4, (c_to // 2) % 2, c_to % 2
        src = rhs.at[pl.ds(j * sub, sub), pl.ds(pl.multiple_of(c_to * ncol, ncol), ncol)]
        dst = state.at[j, pl.ds(pl.multiple_of(col * sub, sub), sub), :]
        return remote(
            src, dst, rhs_send.at[j, c_to], rhs_recv.at[j],
            device(z, x_to, 2 * h_to + low_to, h),
        ), pltpu.make_async_copy(src, dst, rhs_recv.at[j])

    chip = 4 * x + 2 * low + h

    def rhs_stays(c_to):
        return jnp.logical_and(c_to == chip, q == h)

    def send_rhs():
        for j in range(2):

            @pl.loop(0, 16)
            def _(step, j=j):
                c_to = (step + chip) % 16
                away, home = rhs_copy(j, c_to)
                stays = rhs_stays(c_to)

                @pl.when(stays)
                def _():
                    home.start()

                @pl.when(jnp.logical_not(stays))
                def _():
                    away.start()

    pl.when(z < 2)(send_rhs)

    for load in loads:
        load.wait()

    is_diag = col % 8 == row
    diag_slot = col // 8

    def edges(piece, k, dx, dy):
        ways = {0: (dx, k % 2), 2: (dy, (k + k // 2) % 2)}
        first = 2 if FIRST_Y[piece] else 0
        gap, par = ways[first]
        on_line = ways[2 - first][0] == 0
        flags = {
            first: on_line & ((gap == 0) | ((gap == 1) & (par == 0))),
            first + 1: on_line & ((gap == 0) | ((gap == 3) & (par == 1))),
        }
        gap, par = ways[2 - first]
        flags[2 - first] = (gap == 0) | ((gap == 1) & (par == 0))
        flags[3 - first] = (gap == 0) | ((gap == 3) & (par == 1))
        return flags

    def neighbour(way, core):
        if way == 0:
            return device(z, (x + 1) % 4, y, core)
        if way == 1:
            return device(z, (x + 3) % 4, y, core)
        if way == 2:
            return device(z, x, (y + 1) % 4, core)
        return device(z, x, (y + 3) % 4, core)

    def rows_of(piece):
        return pl.ds(piece * part, part)

    def shifts(j, piece):
        return (z >= 2) & (j == 0) & (piece >= PIECES // 2)

    def source_copies(j):
        src = own.at[j]
        for piece in range(PIECES):
            shifted = shifts(j, piece)
            for way in range(6):
                if way < 4:
                    target, flag = neighbour(way, h), jnp.logical_not(shifted)
                elif way == 4:
                    target, flag = device(z, x, y, h), jnp.logical_not(shifted) & (q != h)
                else:
                    target, flag = device(z, (x + 2) % 4, y, h), shifted
                yield flag, remote(
                    src.at[rows_of(piece), :],
                    grid.at[j, col, rows_of(piece), :],
                    source_send.at[j, piece, way],
                    grid_recv.at[j, col, piece],
                    target,
                )

    def source(j):
        for flag, copy in source_copies(j):
            pl.when(flag)(copy.start)

        for piece in range(PIECES):

            @pl.when((q == h) & jnp.logical_not(shifts(j, piece)))
            def _(piece=piece):
                grid[j, col, rows_of(piece), :] = own[j, rows_of(piece), :]

    def source_wait(j):
        for flag, copy in source_copies(j):
            pl.when(flag)(copy.wait_send)

    needed = (col <= row, col <= 8 + row)
    diag_first = is_diag & (diag_slot == 0)
    diag_second = is_diag & (diag_slot == 1)

    pl.when(needed[0] & jnp.logical_not(diag_first))(lambda: source(0))

    @pl.when(is_diag)
    def _():
        invert(own.at[diag_slot], inverse)
        own[diag_slot] = inverse[...]

    pl.when(diag_first)(lambda: source(0))
    reach = (0, 1, 2, 1)
    offsets = sorted(((dx, dy) for dx in range(4) for dy in range(4)), key=lambda o: (reach[o[0]] + 1.5 * reach[o[1]], o[1], o[0]))

    def offset_of(n):
        dx = dy = jnp.int32(0)
        for i, (a, b) in enumerate(offsets):
            dx, dy = jnp.where(n == i, a, dx), jnp.where(n == i, b, dy)
        return dx, dy

    def number_of(dx, dy):
        n = jnp.int32(0)
        for i, (a, b) in enumerate(offsets):
            n = jnp.where((dx == a) & (dy == b), i, n)
        return n

    def passing(j, n, limit, do, after=None):
        dx, dy = offset_of(n)
        x_from, y_from = (x - dx + 4) % 4, (y - dy + 4) % 4
        away = n > 0
        for side in range(2):
            k = 4 * x_from + 2 * (y_from % 2) + side
            for piece in range(PIECES):
                shifted = shifts(j, piece)
                k_piece = jnp.where(shifted, (k + 8) % 16, k)

                @pl.when((y_from // 2 == q) & (k_piece <= limit))
                def _(k=k, k_piece=k_piece, piece=piece, side=side, shifted=shifted):
                    spot = grid.at[j, k_piece, rows_of(piece), :]

                    def copy(way):
                        return remote(spot, spot, pass_send.at[j, k_piece, piece, way], grid_recv.at[j, k_piece, piece], neighbour(way, q))

                    if do == "pass":
                        pl.when(away | (q != side) | shifted)(lambda: copy(0).wait_recv())
                    for way, flag in edges(piece, k, dx, dy).items():

                        @pl.when(flag & (away | shifted))
                        def _(way=way):
                            if do == "pass":
                                copy(way).start()
                            else:
                                copy(way).wait_send()

            if after is not None:
                pl.when((y_from // 2 == q) & (k <= limit))(lambda k=k: after(k))

    ahead = 6 * jnp.maximum(z - 1, 0) // 2
    at_once = z > 1

    pl.when(at_once & needed[1])(lambda: source(1))
    pl.when(z >= 2)(send_rhs)

    @pl.loop(0, 16)
    def _(n):
        passing(0, n, first_row, "pass")

        @pl.loop((n * ahead) // 16, ((n + 1) * ahead) // 16)
        def _(m):
            passing(1, m, second_row, "pass")

    pl.when(jnp.logical_not(at_once) & needed[1])(lambda: source(1))

    for j in range(2):
        remote(state.at[j], state.at[j], rhs_send.at[j, 0], rhs_recv.at[j], here).wait_recv()

    def owner_z(k):
        return (k % 8) // 2

    def wanted(k, z_to):
        return (k < 8) | (z_to > owner_z(k))

    def solved_copies(k):
        spot = solved.at[k]
        partner_wants = jnp.logical_or(k % 2 == 0, k < 8)
        result = []
        for way in range(4):
            if way == 0:
                target, flag = device(z, x, y, 1 - q), partner_wants
            else:
                z_to = (z + (1, 3, 2)[way - 1]) % 4
                target, flag = device(z_to, x, y, 0), wanted(k, z_to)
            result.append((flag, remote(spot, spot, solved_send.at[k, way], solved_recv.at[k], target)))
        return result

    def out_copy(k):
        spot = out.at[pl.ds(pl.multiple_of((k // 8) * nb, nb), nb), :]
        stays = h == q
        target = device(z, x, 2 * q + low, h)
        away = remote(solved.at[k], spot, out_send.at[k // 8], out_recv.at[k // 8], target)
        home = pltpu.make_async_copy(solved.at[k], spot, out_recv.at[k // 8])
        return stays, away, home

    def is_owner(k):
        return jnp.logical_and(owner_z(k) == z, k % 2 == q)

    def pass_to_partner(k):
        spot = solved.at[k]
        flag = jnp.logical_and(q == 0, jnp.logical_and(owner_z(k) != z, wanted(k, z)))
        return flag, remote(spot, spot, solved_pass.at[k], solved_recv.at[k], device(z, x, y, 1))

    def gets(k):
        same_chip = owner_z(k) == z
        other_core = jnp.logical_and(same_chip, jnp.logical_and(k % 2 != q, jnp.logical_or(k % 2 == 0, k < 8)))
        return jnp.logical_or(other_core, jnp.logical_and(jnp.logical_not(same_chip), wanted(k, z)))

    def solve(k):
        slot = k // 8
        solved[k] = product(grid[slot, k], state[slot])
        for flag, copy in solved_copies(k):
            pl.when(flag)(copy.start)
        stays, away, home = out_copy(k)
        pl.when(stays)(home.start)
        pl.when(jnp.logical_not(stays))(away.start)

    def update(slot, k):
        state[slot] = state[slot] - product(grid[slot, k], solved[k])

    def passed(k):
        return jnp.where(k <= 2 * z, ahead, jnp.minimum(jnp.maximum(10 + k - 2 * z, ahead), 16))

    @pl.loop(-1, 16)
    def _(k):
        @pl.when((k >= 0) & gets(k))
        def _():
            spot = solved.at[k]
            remote(spot, spot, solved_pass.at[k], solved_recv.at[k], here).wait_recv()
            flag, copy = pass_to_partner(k)
            pl.when(flag)(copy.start)

        k_y = 2 * q + (k // 2) % 2
        taken = number_of((x - k // 4 + 4) % 4, (y - k_y + 4) % 4) < passed(k)
        early = (k >= 0) & (k < first_row)
        late = (k >= 0) & (k < second_row) & taken
        near = (k + 1) // 8

        @pl.when(jnp.where(k < 7, early, late) & (k < 15))
        def _():
            update(near, k)

        pl.when(is_owner(k + 1) & (k < 15))(lambda: solve(k + 1))

        @pl.when((k < 7) & late)
        def _():
            update(1, k)

        @pl.when(k >= 0)
        def _():
            def after(column):
                pl.when((column <= k) & (column < second_row))(lambda: update(1, column))

            @pl.loop(passed(k), passed(k + 1))
            def _(n):
                passing(1, n, second_row, "pass", after)

    @pl.loop(0, 16)
    def _(k):
        @pl.when(is_owner(k))
        def _():
            for flag, copy in solved_copies(k):

                @pl.when(flag)
                def _(copy=copy):
                    copy.wait_send()

            stays, away, _ = out_copy(k)

            @pl.when(jnp.logical_not(stays))
            def _():
                away.wait_send()

        flag, copy = pass_to_partner(k)

        @pl.when(flag)
        def _():
            copy.wait_send()

    @pl.loop(0, 16)
    def _(n):
        passing(0, n, first_row, "done")
        passing(1, n, second_row, "done")

    for j in range(2):
        pl.when(needed[j])(lambda j=j: source_wait(j))

    for j in range(2):

        @pl.loop(0, 16)
        def _(c_to, j=j):
            away, _ = rhs_copy(j, c_to)

            @pl.when(jnp.logical_not(rhs_stays(c_to)))
            def _():
                away.wait_send()

        spot = out.at[pl.ds(j * nb, nb), :]
        remote(solved.at[0], spot, out_send.at[j], out_recv.at[j], here).wait_recv()


def on_device(tri, rhs):
    nb = tri.shape[1]
    ncol = rhs.shape[1] // 16
    dma = pltpu.SemaphoreType.DMA
    return pl.pallas_call(
        kernel,
        out_shape=jax.ShapeDtypeStruct((2 * nb, ncol), F32),
        in_specs=[pl.BlockSpec(memory_space=pl.ANY)] * 2,
        out_specs=pl.BlockSpec(memory_space=pl.ANY),
        scratch_shapes=[
            pltpu.VMEM((2, 16, nb, nb), F32),
            pltpu.VMEM((2, nb, nb), F32),
            pltpu.VMEM((nb, nb), F32),
            pltpu.VMEM((16, nb, ncol), F32),
            pltpu.VMEM((2, nb, ncol), F32),
            dma((2,)),
            dma((2, 16)),
            dma((2,)),
            dma((2, 16, PIECES)),
            dma((2, PIECES, 6)),
            dma((2, 16, PIECES, 4)),
            dma((16, 4)),
            dma((16,)),
            dma((16,)),
            dma((2,)),
            dma((2,)),
        ],
        compiler_params=pltpu.CompilerParams(
            collective_id=0, has_side_effects=True, vmem_limit_bytes=60 * 1024 * 1024
        ),
    )(tri, rhs)


def solution(mesh):
    return jax.shard_map(
        on_device,
        mesh=mesh,
        in_specs=(P("row", "col"), P(("row", "col"), None)),
        out_specs=P("row", "col"),
        check_vma=False,
    )
```
